32 devices in a mesh: row: 4 (over z), col: 8 (over y, x, core).
Axes of the slice: x: 2, y: 2, z: 4, core: 2. Of those that a mesh axis runs over, the one named last changes fastest.
Arguments:
- front: float32 [12288, 12288], P('row', 'col'), as said below
- structure: int32 [3, 96], replicated, may hold values from 0 to 1, as said below
- factor_front: float32 [3, 12288, 512], P(None, 'row', 'col'), may hold values from -0.0546875 to 0.0546875
- factor_border: float32 [2, 512, 512], replicated, may hold values from -0.6 to 0.6
- pivot_inverse: float32 [3, 512, 512], P(None, 'row')
Outputs:
- inverse_front: float32 [3, 512, 12288], P(None, 'row', 'col')
- inverse_parent: float32 [2, 512, 512], P(None, 'row')
- inverse_diagonal: float32 [3, 512, 512], P(None, 'row')
The draws below stay inside these ranges and needn't reach their ends.
Inputs may be any that keep to these rules, and one draw needn't show every extreme that they name: front is exactly symmetric. structure[k, b] = 1 where front block b (rows b * 128 to (b + 1) * 128 - 1) lies in supernode k's structure; every 1 in row k is also a 1 in row k - 1; blocks b < 24 are 1 in every row.
All inputs are finite; a program needn't handle non-finite values.
Results may differ from the reference program's by a relative error of at most 0.0001.
Values sent between devices are 32-bit elements; how exact they have to be, the bound alone decides.
No kernel may reach another device: no remote copies, remote signals or barrier semaphores. Data moves between devices by JAX's collectives and lax.ppermute only.
A program may use at most 128 MiB of HBM per device.

```python
import jax
import jax.numpy as jnp
from jax import lax

F = 12288
W = 512
BLK = 128
SUPER = 3
NBLK = 96


def draw_front(key, part):
    noise_part = jax.random.normal(jax.random.fold_in(key, 11), (F, F), jnp.float32) * 0.02
    symmetric = (noise_part + noise_part.T) * 0.5
    diagonal = jnp.exp(jax.random.uniform(jax.random.fold_in(key, 12), (F,), jnp.float32, jnp.log(4.0), jnp.log(16.0)))
    return symmetric + jnp.diag(diagonal)


def draw_pivot_inverse(key, part):
    noise_part = jax.random.normal(jax.random.fold_in(key, 31), (SUPER, W, W), jnp.float32) * (0.5 / W ** 0.5)
    symmetric = (noise_part + jnp.swapaxes(noise_part, 1, 2)) * 0.5
    diagonal = jnp.exp(jax.random.uniform(jax.random.fold_in(key, 32), (SUPER, W), jnp.float32, jnp.log(1.0), jnp.log(4.0)))
    return symmetric + diagonal[:, :, None] * jnp.eye(W, dtype=jnp.float32)[None, :, :]


def draw_structure(key, part):
    draws = jax.random.randint(jax.random.fold_in(key, 21), (NBLK,), 0, 1000)
    numbers = jnp.arange(NBLK, dtype=jnp.int32)
    levels = 200 + 700 * numbers // NBLK
    sections = jnp.arange(SUPER, dtype=jnp.int32)
    listed = draws[None, :] * (SUPER + 1) < levels[None, :] * (SUPER + 1 - sections[:, None])
    forced = (numbers < NBLK // 4)[None, :]
    return jnp.logical_or(listed, forced).astype(jnp.int32)


def block_scale(rng, shape, pieces, smallest, top_value):
    factor_of = 1.0
    for axis_at, shards_of in pieces:
        steps = jax.random.uniform(jax.random.fold_in(jax.random.fold_in(rng, 6), axis_at), (shards_of,), jnp.float32, smallest / len(pieces), top_value / len(pieces))
        factor_of = factor_of * jnp.repeat(jnp.exp(steps), shape[axis_at] // shards_of).reshape((-1,) + (1,) * (len(shape) - 1 - axis_at))
    return factor_of


def noise(own_key, extent, spread, limit, pieces=(), kind=jnp.bfloat16):
    loudness = block_scale(own_key, extent, pieces, -0.22, 0.18) if pieces else 1.0
    array = jax.random.normal(own_key, extent, jnp.float32) * spread * loudness
    return jnp.minimum(jnp.maximum(array, -limit), limit).astype(kind)


def setup_inputs(seed: int = 0) -> dict:
    streams_of = jax.random.split(jax.random.key(seed), 6)
    front = draw_front(jax.random.fold_in(streams_of[5], 71), 0)
    structure = draw_structure(jax.random.fold_in(streams_of[5], 71), 0)
    factor_front = noise(streams_of[2], (SUPER, F, W), F ** -0.5, 0.0546875, ((1, 4), (2, 8)), jnp.float32)
    factor_border = noise(streams_of[3], (SUPER - 1, W, W), 0.1, 0.6, (), jnp.float32)
    pivot_inverse = draw_pivot_inverse(jax.random.fold_in(streams_of[5], 71), 0)
    return dict(front=front, structure=structure, factor_front=factor_front, factor_border=factor_border, pivot_inverse=pivot_inverse)


HIGH = lax.Precision.HIGHEST


def matmul(former, latter):
    return jnp.dot(former, latter, precision=HIGH, preferred_element_type=jnp.float32)


def reference(front, structure, factor_front, factor_border, pivot_inverse):
    supers = structure.shape[0]
    order = front.shape[0]
    owners = (jnp.arange(order, dtype=jnp.int32) // BLK).astype(jnp.int32)
    fronts = []
    parents = []
    diagonals = []
    previous = None
    diag_prev = None
    for section in range(supers):
        flags = structure[section][owners].astype(jnp.float32)
        factor_rows = factor_front[section] * flags[:, None]
        image = matmul(front, factor_rows)
        if section > 0:
            border = factor_border[section - 1]
            image = image + matmul(previous, border)
            parent = matmul(previous.T, factor_rows) + matmul(diag_prev, border)
            parents.append(-parent)
        current = -(image * flags[:, None])
        diag_now = pivot_inverse[section] + matmul(image.T, factor_rows)
        if section > 0:
            diag_now = diag_now + matmul(parent.T, border)
        fronts.append(current.T)
        diagonals.append(diag_now)
        previous = current
        diag_prev = diag_now
    return jnp.stack(fronts), jnp.stack(parents), jnp.stack(diagonals)
```

```python
import jax
import jax.numpy as jnp
from jax import lax
from jax.sharding import PartitionSpec as P


BLK = 128
HALVES = 2

HIGH = lax.Precision.HIGH


def contract(former, latter, former_dim, latter_dim):
    return lax.dot_general(
        former,
        latter,
        (((former_dim,), (latter_dim,)), ((), ())),
        precision=HIGH,
        preferred_element_type=jnp.float32,
    )


def swap(x, axis, bit):
    size = lax.axis_size(axis)
    return lax.ppermute(x, axis, [(i, i ^ bit) for i in range(size)])


def bits_of(size):
    return [1 << i for i in range(size.bit_length() - 1)]


def local_flags(structure, index, count):
    blocks = count // BLK
    mine = lax.dynamic_slice_in_dim(structure, index * blocks, blocks, 1)
    mine = mine.astype(jnp.float32)[:, :, None]
    return jnp.broadcast_to(mine, mine.shape[:2] + (BLK,)).reshape(structure.shape[0], count)


def absolute(pieces, index):
    pieces = [p[None] for p in pieces]
    bit = 1
    while len(pieces) > 1:
        mine = (index // bit) % 2 == 1
        pieces = [
            jnp.concatenate([jnp.where(mine, h, l), jnp.where(mine, l, h)], axis=0)
            for l, h in zip(pieces[::2], pieces[1::2])
        ]
        bit *= 2
    return pieces[0]


def relay(x, axis):
    index = lax.axis_index(axis)
    x = x[None]
    for bit in bits_of(lax.axis_size(axis)):
        got = swap(x, axis, bit)
        mine = (index // bit) % 2 == 1
        x = jnp.concatenate([jnp.where(mine, got, x), jnp.where(mine, x, got)], axis=0)
    return x


def direct(x, axis, join):
    size = lax.axis_size(axis)
    even = [x] + [swap(x, axis, k) for k in range(2, size, 2)]
    even = jnp.concatenate(even, axis=join)
    return even, swap(even, axis, 1)


def quick(x, axis):
    size = lax.axis_size(axis)
    if size != 8:
        even, odd = direct(x[None], axis, 0)
        return [(even, odd)[j % 2][j // 2] for j in range(size)]
    cut = x.shape[0] // 2
    near = {0: x}
    for k in (2, 4):
        near[k] = swap(x, axis, k)
    sides = {1: swap(x, axis, 1)}
    near[6] = jnp.concatenate(
        [swap(near[4][:cut], axis, 2), swap(near[2][cut:], axis, 4)], axis=0
    )
    for k in (2, 4, 6):
        sides[k + 1] = swap(near[k], axis, 1)
    near.update(sides)
    return [near[k] for k in range(size)]


def scatter_sum(x, axis):
    index = lax.axis_index(axis)
    got = None
    for bit in bits_of(lax.axis_size(axis)):
        if got is not None:
            x = x + got
        x = x.reshape((x.shape[0] // 2, 2) + x.shape[1:])
        mine = (index // bit) % 2
        send = lax.dynamic_index_in_dim(x, 1 - mine, 1, keepdims=False)
        x = lax.dynamic_index_in_dim(x, mine, 1, keepdims=False)
        got = swap(send, axis, bit)
    return (x + got)[0]


def exchange(x, axis):
    size = lax.axis_size(axis)
    index = lax.axis_index(axis)
    sent = [lax.dynamic_index_in_dim(x, index ^ k, 0, keepdims=False) for k in range(size)]
    sent = lax.optimization_barrier(tuple(sent))
    got = [sent[0]] + [swap(sent[k], axis, k) for k in range(1, size)]
    return absolute(lax.optimization_barrier(tuple(got)), index)


def chain(front, structure, factor_front, factor_border, pivot_inverse):
    rows = lax.axis_size("row")
    cols = lax.axis_size("col")
    row_index = lax.axis_index("row")
    col_index = lax.axis_index("col")
    rows_here, cols_here = front.shape
    supers, width_here, width = pivot_inverse.shape
    fine = width_here // cols
    ratio = cols // rows
    part_cols = cols_here // HALVES
    row_flags = local_flags(structure, row_index, rows_here)
    col_flags = local_flags(structure, col_index, cols_here)

    own = [factor_front[k].T * row_flags[k][None, :] for k in range(supers)]
    factors = []
    for k in range(supers):
        if k == 0:
            pieces = quick(own[k], "col")
        else:
            even, odd = direct(own[k][None], "col", 0)
            pieces = [(even, odd)[j % 2][j // 2] for j in range(cols)]
        factors.append(absolute(pieces, col_index).reshape(width, rows_here))

    fronts = []
    partial_prev = None
    for k in range(supers):
        part = contract(factors[k], front, 1, 0)
        if k > 0:
            part = part - contract(factor_border[k - 1], partial_prev, 0, 0)
        partial_prev = part
        parts = []
        for h in range(HALVES):
            x = part[:, h * part_cols : (h + 1) * part_cols].reshape(rows, width_here, part_cols)
            x = scatter_sum(x, "row")
            parts.append(-(x * col_flags[k][None, h * part_cols : (h + 1) * part_cols]))
        fronts.append(jnp.concatenate(parts, axis=1))

    products = []
    for k in range(supers):
        spread = exchange(fronts[k].reshape(cols, fine, cols_here), "col")
        spread = spread.reshape(rows, ratio, fine, cols_here)
        lines = exchange(spread, "row")
        lines = jnp.swapaxes(lines, 1, 2).reshape(rows * fine, rows_here)
        products.append([contract(lines, f, 1, 1) for f in factors[k : k + 2]])
    grams = {}
    for members in (range(supers - 1), range(supers - 1, supers)):
        keys = [(k, k + j) for k in members for j in range(len(products[k]))]
        got = jnp.stack([products[k][m - k] for k, m in keys], axis=1)
        got = scatter_sum(got.reshape(rows, fine, len(keys), width), "row")
        got = relay(got, "col").reshape(width_here, len(keys), width)
        grams.update({key: got[:, i] for i, key in enumerate(keys)})

    parents = []
    diagonals = []
    for k in range(supers):
        diag = pivot_inverse[k] - grams[k, k]
        if k > 0:
            border = factor_border[k - 1]
            parent = grams[k - 1, k] + contract(diagonals[k - 1], border, 1, 0)
            parents.append(-parent)
            slots = jnp.swapaxes(parent.reshape(width_here, rows, width_here), 0, 1)
            sliver = exchange(slots, "row").reshape(width, width_here)
            diag = diag + contract(sliver, border, 0, 0)
        diagonals.append(diag)
    return (jnp.stack(fronts), jnp.stack(parents), jnp.stack(diagonals))


def solution(mesh):
    placed = (P("row", "col"), P(), P(None, "row", "col"), P(), P(None, "row", None))
    return jax.shard_map(
        chain,
        mesh=mesh,
        in_specs=placed,
        out_specs=(P(None, "row", "col"), P(None, "row", None), P(None, "row", None)),
        check_vma=False,
    )
```

```python
import jax
import jax.numpy as jnp
from jax import lax
from jax.sharding import PartitionSpec as P


BLK = 128
HALVES = 2

HIGH = lax.Precision.HIGH


def contract(former, latter, former_dim, latter_dim):
    return lax.dot_general(
        former,
        latter,
        (((former_dim,), (latter_dim,)), ((), ())),
        precision=HIGH,
        preferred_element_type=jnp.float32,
    )


def swap(x, axis, bit):
    size = lax.axis_size(axis)
    return lax.ppermute(x, axis, [(i, i ^ bit) for i in range(size)])


def bits_of(size):
    return [1 << i for i in range(size.bit_length() - 1)]


def local_flags(structure, index, count):
    blocks = count // BLK
    mine = lax.dynamic_slice_in_dim(structure, index * blocks, blocks, 1)
    mine = mine.astype(jnp.float32)[:, :, None]
    return jnp.broadcast_to(mine, mine.shape[:2] + (BLK,)).reshape(structure.shape[0], count)


def absolute(pieces, index):
    pieces = [p[None] for p in pieces]
    bit = 1
    while len(pieces) > 1:
        mine = (index // bit) % 2 == 1
        pieces = [
            jnp.concatenate([jnp.where(mine, h, l), jnp.where(mine, l, h)], axis=0)
            for l, h in zip(pieces[::2], pieces[1::2])
        ]
        bit *= 2
    return pieces[0]


def relay(x, axis):
    index = lax.axis_index(axis)
    x = x[None]
    for bit in bits_of(lax.axis_size(axis)):
        got = swap(x, axis, bit)
        mine = (index // bit) % 2 == 1
        x = jnp.concatenate([jnp.where(mine, got, x), jnp.where(mine, x, got)], axis=0)
    return x


def direct(x, axis):
    size = lax.axis_size(axis)
    near = {k: swap(x, axis, k) if k else x for k in range(0, size, 2)}
    near.update({k + 1: swap(near[k], axis, 1) for k in range(0, size, 2)})
    return [near[k] for k in range(size)]


def quick(x, axis):
    size = lax.axis_size(axis)
    if size != 8:
        return direct(x, axis)
    cut = x.shape[0] // 2
    near = {0: x}
    for k in (2, 4):
        near[k] = swap(x, axis, k)
    sides = {1: swap(x, axis, 1)}
    near[6] = jnp.concatenate([swap(near[4][:cut], axis, 2), swap(near[2][cut:], axis, 4)], axis=0)
    for k in (2, 4, 6):
        sides[k + 1] = swap(near[k], axis, 1)
    near.update(sides)
    return [near[k] for k in range(size)]


def scatter_sum(x, axis):
    index = lax.axis_index(axis)
    got = None
    for bit in bits_of(lax.axis_size(axis)):
        if got is not None:
            x = x + got
        x = x.reshape((x.shape[0] // 2, 2) + x.shape[1:])
        mine = (index // bit) % 2
        send = lax.dynamic_index_in_dim(x, 1 - mine, 1, keepdims=False)
        x = lax.dynamic_index_in_dim(x, mine, 1, keepdims=False)
        got = swap(send, axis, bit)
    return (x + got)[0]


def exchange(x, axis):
    size = lax.axis_size(axis)
    index = lax.axis_index(axis)
    sent = [lax.dynamic_index_in_dim(x, index ^ k, 0, keepdims=False) for k in range(size)]
    sent = lax.optimization_barrier(tuple(sent))
    got = [sent[0]] + [swap(sent[k], axis, k) for k in range(1, size)]
    return absolute(lax.optimization_barrier(tuple(got)), index)


def chain(front, structure, factor_front, factor_border, pivot_inverse):
    rows = lax.axis_size("row")
    cols = lax.axis_size("col")
    row_index = lax.axis_index("row")
    col_index = lax.axis_index("col")
    rows_here, cols_here = front.shape
    supers, width_here, width = pivot_inverse.shape
    fine = width_here // cols
    ratio = cols // rows
    part_cols = cols_here // HALVES
    row_flags = local_flags(structure, row_index, rows_here)
    col_flags = local_flags(structure, col_index, cols_here)

    own = [factor_front[k].T * row_flags[k][None, :] for k in range(supers)]
    factors = []
    for k in range(supers):
        if k == 0:
            pieces = quick(own[k], "col")
        else:
            pieces = direct(own[k], "col")
        factors.append(absolute(pieces, col_index).reshape(width, rows_here))

    fronts = []
    partial_prev = None
    for k in range(supers):
        part = contract(factors[k], front, 1, 0)
        if k > 0:
            part = part - contract(factor_border[k - 1], partial_prev, 0, 0)
        partial_prev = part
        parts = []
        for h in range(HALVES):
            x = part[:, h * part_cols : (h + 1) * part_cols].reshape(rows, width_here, part_cols)
            x = scatter_sum(x, "row")
            parts.append(-(x * col_flags[k][None, h * part_cols : (h + 1) * part_cols]))
        fronts.append(jnp.concatenate(parts, axis=1))

    products = []
    for k in range(supers):
        spread = exchange(fronts[k].reshape(cols, fine, cols_here), "col")
        spread = spread.reshape(rows, ratio, fine, cols_here)
        lines = exchange(spread, "row")
        lines = jnp.swapaxes(lines, 1, 2).reshape(rows * fine, rows_here)
        products.append([contract(lines, f, 1, 1) for f in factors[k : k + 2]])
    grams = {}
    for k in range(supers):
        count = len(products[k])
        got = jnp.stack(products[k], axis=1).reshape(rows, fine, count, width)
        got = scatter_sum(got, "row")
        got = relay(got, "col").reshape(width_here, count, width)
        grams.update({(k, k + j): got[:, j] for j in range(count)})

    parents = []
    diagonals = []
    for k in range(supers):
        diag = pivot_inverse[k] - grams[k, k]
        if k > 0:
            border = factor_border[k - 1]
            parent = grams[k - 1, k] + contract(diagonals[k - 1], border, 1, 0)
            parents.append(-parent)
            slots = jnp.swapaxes(parent.reshape(width_here, rows, width_here), 0, 1)
            sliver = exchange(slots, "row").reshape(width, width_here)
            diag = diag + contract(sliver, border, 0, 0)
        diagonals.append(diag)
    return (jnp.stack(fronts), jnp.stack(parents), jnp.stack(diagonals))


def solution(mesh):
    placed = (P("row", "col"), P(), P(None, "row", "col"), P(), P(None, "row", None))
    return jax.shard_map(
        chain,
        mesh=mesh,
        in_specs=placed,
        out_specs=(P(None, "row", "col"), P(None, "row", None), P(None, "row", None)),
        check_vma=False,
    )
```
